128 devices in a mesh: rows: 16 (over y, z), dp: 8 (over x, core).
Axes of the slice: x: 4, y: 4, z: 4, core: 2. Of those that a mesh axis runs over, the one named last changes fastest.
Arguments:
- weights: float32 [24576, 4096], P(('rows', 'dp'))
- moment: float32 [24576, 4096], P(('rows', 'dp'))
- second: float32 [24576, 4096], P(('rows', 'dp')), may hold values from 0.01 to 1
- tile_rows: bfloat16 [32768, 4096], P(('rows', 'dp')), may hold values from -6 to 6
- row_index: int32 [32768], P(('rows', 'dp')), may hold values from 0 to 191
- bucket_count: int32 [16384], P(('rows', 'dp')), may hold values from 1 to 2, as said below
Outputs:
- new_weights: float32 [24576, 4096], P(('rows', 'dp'))
- new_moment: float32 [24576, 4096], P(('rows', 'dp'))
- new_second: float32 [24576, 4096], P(('rows', 'dp'))
The draws below stay inside these ranges and needn't reach their ends.
Inputs may be any that keep to these rules, and one draw needn't show every extreme that they name: `bucket_count`: at least one slot of every sender and owner is live; in every draw some owner receives 2 live slots from every sender. `row_index`: rows may repeat within and across senders.
All inputs are finite; a program needn't handle non-finite values.
Results may differ from the reference program's by a relative error of at most 0.0003.
Values may be sent and summed in bfloat16 or wider, within the bound.
No kernel may reach another device: no remote copies, remote signals or barrier semaphores. Data moves between devices by JAX's collectives and lax.ppermute only.
A program may use at most 64 MiB of HBM per device.

```python
import math
import jax
import jax.numpy as jnp

D = 4096
ROWS_DEV = 192
CAP = 2
OWNERS = 128
VOCAB = 24576
SLOTS = 256


def draw_weights(key, part):
    key_one = jax.random.fold_in(key, 21)
    key_two = jax.random.fold_in(key, 22)
    key_three = jax.random.fold_in(key, 23)
    row_pos = jnp.arange(VOCAB, dtype=jnp.float32) / VOCAB
    normal_part = jax.random.truncated_normal(key_one, -4.0, 4.0, (VOCAB, D), jnp.float32)
    row_scale = 10.0 ** jax.random.uniform(key_two, (VOCAB, 1), jnp.float32) * 3.0 ** row_pos[:, None]
    col_scale = 10.0 ** jax.random.uniform(key_three, (1, D), jnp.float32)
    return 0.05 * normal_part * row_scale * col_scale


def draw_moment(key, part):
    key_one = jax.random.fold_in(key, 31)
    key_two = jax.random.fold_in(key, 32)
    row_pos = jnp.arange(VOCAB, dtype=jnp.float32) / VOCAB
    normal_part = jax.random.truncated_normal(key_one, -4.0, 4.0, (VOCAB, D), jnp.float32)
    row_scale = 10.0 ** jax.random.uniform(key_two, (VOCAB, 1), jnp.float32) * 3.0 ** row_pos[:, None]
    return 0.05 * normal_part * row_scale


def draw_bucket_count(key, part):
    key_one = jax.random.fold_in(key, 11)
    key_two = jax.random.fold_in(key, 12)
    counts_all = jax.random.randint(key_one, (OWNERS, OWNERS), 1, CAP + 1)
    full_owner = jax.random.randint(key_two, (), 0, OWNERS)
    column_id = jnp.arange(OWNERS)[None, :]
    return jnp.where(column_id == full_owner, CAP, counts_all).reshape(-1).astype(jnp.int32)


def touch_ends(entries, stream_key, least, largest):
    spot = [jax.random.randint(jax.random.fold_in(stream_key, axis), (), 0, length) for axis, length in enumerate(entries.shape)]
    widest = entries.shape.index(max(entries.shape))
    next_to = spot[:widest] + [(spot[widest] + 1) % entries.shape[widest]] + spot[widest + 1:]
    return entries.at[tuple(spot)].set(least).at[tuple(next_to)].set(largest)


def steps_of(stream_key, extent, split, least, largest):
    factor_of = 1.0
    for dim, shards_of in split:
        steps = jax.random.uniform(jax.random.fold_in(jax.random.fold_in(stream_key, 6), dim), (shards_of,), jnp.float32, least / len(split), largest / len(split))
        factor_of = factor_of * jnp.repeat(jnp.exp(steps), extent[dim] // shards_of).reshape((-1,) + (1,) * (len(extent) - 1 - dim))
    return factor_of


def gaussian(stream_key, extent, scale, limit, shards=(), kind=jnp.bfloat16):
    loudness = steps_of(stream_key, extent, shards, -0.22, 0.18) if shards else 1.0
    array = jax.random.normal(stream_key, extent, jnp.float32) * scale * loudness
    return jnp.minimum(jnp.maximum(array, -limit), limit).astype(kind)


def setup_inputs(seed: int = 0) -> dict:
    streams_of = jax.random.split(jax.random.key(seed), 7)
    return {
        "weights": draw_weights(jax.random.fold_in(streams_of[6], 71), 0),
        "moment": draw_moment(jax.random.fold_in(streams_of[6], 71), 0),
        "second": jnp.clip(jnp.exp(math.log(1.0) - 4.6051702 * jax.random.uniform(streams_of[2], (VOCAB, D), jnp.float32) ** steps_of(streams_of[2], (VOCAB, D), ((0, 128),), -0.2, 0.2)), 0.01, 1.0),
        "tile_rows": gaussian(streams_of[3], (OWNERS * SLOTS, D), 1.0, 6.0, ((0, 128),)),
        "row_index": touch_ends(jax.random.randint(streams_of[4], (OWNERS * SLOTS,), 0, ROWS_DEV), jax.random.fold_in(streams_of[4], 1), 0, ROWS_DEV - 1).astype(jnp.int32),
        "bucket_count": draw_bucket_count(jax.random.fold_in(streams_of[6], 71), 0),
    }


beta_one = 0.9
beta_two = 0.999
epsilon = 1e-06
decay = 0.01
rate = 0.1

def reference(weights, moment, second, tile_rows, row_index, bucket_count):
    position = jnp.arange(OWNERS * SLOTS, dtype=jnp.int32)
    slot_pos = position % CAP
    bucket_id = position // CAP
    owner_id = bucket_id % OWNERS
    is_live = slot_pos < bucket_count[bucket_id]
    table_row = jnp.where(is_live, owner_id * ROWS_DEV + row_index, 0).astype(jnp.int32)
    values = tile_rows.astype(jnp.float32) * is_live.astype(jnp.float32)[:, None]
    gradient = jax.ops.segment_sum(values, table_row, num_segments=VOCAB)
    new_moment = beta_one * moment + (1.0 - beta_one) * gradient
    new_second = beta_two * second + (1.0 - beta_two) * gradient * gradient
    update = new_moment / (jnp.sqrt(new_second) + epsilon) + decay * weights
    weight_sq = jnp.sum(weights * weights)
    update_sq = jnp.sum(update * update)
    trust_ratio = jnp.sqrt(weight_sq) / jnp.sqrt(update_sq + 1e-06)
    new_weights = weights - rate * trust_ratio * update
    return (new_weights, new_moment, new_second)
```

```python
import jax
import jax.numpy as jnp
from jax import lax
from jax.experimental import pallas as pl
from jax.experimental.pallas import tpu as pltpu
from jax.sharding import Mesh
from jax.sharding import PartitionSpec as P

AXES = ("rows_0", "rows_1", "dp_0", "dp_1")

beta_one = 0.9
beta_two = 0.999
epsilon = 1e-06
decay = 0.01
rate = 0.1

LANES = 128
VMEM_LIMIT = 20 * 1024 * 1024

any_spec = pl.BlockSpec(memory_space=pl.ANY)
vmem_spec = pl.BlockSpec(memory_space=pltpu.VMEM)
hbm_spec = pl.BlockSpec(memory_space=pltpu.HBM)


def pack_body(rows, index, count, packed, sem):
    owners, capacity, width = packed.shape
    width -= LANES
    slots = owners * capacity
    for b in range(owners):
        pltpu.make_async_copy(
            rows.at[pl.ds(b * capacity, capacity)], packed.at[b, :, pl.ds(0, width)], sem
        ).start()
    at = lax.broadcasted_iota(jnp.int32, (slots, slots), 0)
    spread = jnp.where(at == lax.broadcasted_iota(jnp.int32, (slots, slots), 1), index[...], 0)
    of = lax.broadcasted_iota(jnp.int32, (slots, owners), 0) // capacity
    counts = jnp.where(of == lax.broadcasted_iota(jnp.int32, (slots, owners), 1), count[...], 0)

    def along_lanes(x):
        x = x.astype(jnp.float32).astype(jnp.bfloat16)
        return jnp.dot(x, jnp.ones((x.shape[1], LANES), jnp.bfloat16), preferred_element_type=jnp.float32)

    slot = (lax.broadcasted_iota(jnp.int32, (slots, LANES), 0) % capacity).astype(jnp.float32)
    target = jnp.where(slot < along_lanes(counts), along_lanes(spread), -1.0)
    packed[:, :, pl.ds(width, LANES)] = target.astype(jnp.bfloat16).reshape(owners, capacity, LANES)
    whole = packed.at[:, :, pl.ds(0, width)]
    pltpu.make_async_copy(whole, whole, sem).wait()


def pack(rows, index, count, owners):
    slots, width = rows.shape
    return pl.pallas_call(
        pack_body,
        out_shape=pltpu.VMEM((owners, slots // owners, width + LANES), jnp.bfloat16),
        in_specs=[hbm_spec, vmem_spec, vmem_spec],
        out_specs=vmem_spec,
        scratch_shapes=[pltpu.SemaphoreType.DMA],
        compiler_params=pltpu.CompilerParams(vmem_limit_bytes=VMEM_LIMIT),
        name="pack",
    )(rows, index.reshape(1, slots), count.reshape(1, owners))


CHUNK = 512


def step_body(got, w, m, v, nm_hbm, nv_hbm, u, parts, nm, nv, sems):
    owners, capacity, width = got.shape
    width -= LANES
    slots = owners * capacity
    rows = w.shape[0]
    targets = got[:, :, pl.ds(width, LANES)].reshape(slots, LANES)
    first = (lax.broadcasted_iota(jnp.int32, (8, LANES), 1) == 0).astype(jnp.float32).astype(jnp.bfloat16)
    landing = lax.dot_general(first, targets, (((1,), (1,)), ((), ())), preferred_element_type=jnp.float32)
    row = lax.broadcasted_iota(jnp.int32, (rows, slots), 0).astype(jnp.float32)
    picker = jnp.where(landing[:1, :] == row, 1.0, 0.0).astype(jnp.bfloat16)
    update_sq = jnp.zeros((8, LANES), jnp.float32)
    weight_sq = jnp.zeros((8, LANES), jnp.float32)

    def add_squares(total, x):
        sq = (x * x).reshape(rows // 8, 8, CHUNK).sum(axis=0)
        for i in range(CHUNK // LANES):
            total = total + sq[:, i * LANES : (i + 1) * LANES]
        return total

    for j in range(width // CHUNK):
        at = pl.ds(j * CHUNK, CHUNK)
        arrived = got[:, :, at].reshape(slots, CHUNK)
        g = jnp.dot(picker, arrived, preferred_element_type=jnp.float32)
        new_m = beta_one * m[:, at] + (1.0 - beta_one) * g
        new_v = beta_two * v[:, at] + (1.0 - beta_two) * g * g
        old_w = w[:, at]
        update = new_m / (jnp.sqrt(new_v) + epsilon) + decay * old_w
        nm[:, at] = new_m
        nv[:, at] = new_v
        u[:, at] = update
        for k, (a, b) in enumerate(((nm, nm_hbm), (nv, nv_hbm))):
            pltpu.make_async_copy(a.at[:, at], b.at[:, at], sems.at[k]).start()
        update_sq = add_squares(update_sq, update)
        weight_sq = add_squares(weight_sq, old_w)
    both = jnp.concatenate([x.sum(axis=0, keepdims=True) for x in (update_sq, weight_sq)], axis=1)
    parts[...] = jnp.broadcast_to(both[None], parts.shape)
    for k, (a, b) in enumerate(((nm, nm_hbm), (nv, nv_hbm))):
        pltpu.make_async_copy(a, b, sems.at[k]).wait()


def step(got, w, m, v, peers):
    table = jax.ShapeDtypeStruct(w.shape, jnp.float32)
    return pl.pallas_call(
        step_body,
        out_shape=[table, table, pltpu.VMEM(w.shape, jnp.float32), pltpu.VMEM((peers, 1, 2 * LANES), jnp.float32)],
        in_specs=[vmem_spec] * 4,
        out_specs=[hbm_spec, hbm_spec, vmem_spec, vmem_spec],
        scratch_shapes=[
            pltpu.VMEM(w.shape, jnp.float32),
            pltpu.VMEM(w.shape, jnp.float32),
            pltpu.SemaphoreType.DMA((2,)),
        ],
        compiler_params=pltpu.CompilerParams(vmem_limit_bytes=VMEM_LIMIT),
        name="step",
    )(got, w, m, v)


def finish_body(parts, u, w, out_hbm, out, sem):
    sums = parts[...].reshape(parts.shape[0], parts.shape[2]).sum(axis=0, keepdims=True)
    update_sq = jnp.sum(sums[:, :LANES], axis=1, keepdims=True)
    weight_sq = jnp.sum(sums[:, LANES:], axis=1, keepdims=True)
    scale = rate * (jnp.sqrt(weight_sq) / jnp.sqrt(update_sq + 1e-06))
    for i in range(out.shape[0] // 32):
        at = pl.ds(i * 32, 32)
        out[at, :] = w[at, :] - scale * u[at, :]
        pltpu.make_async_copy(out.at[at, :], out_hbm.at[at, :], sem).start()
    pltpu.make_async_copy(out, out_hbm, sem).wait()


def finish(parts, u, w):
    return pl.pallas_call(
        finish_body,
        out_shape=jax.ShapeDtypeStruct(w.shape, jnp.float32),
        in_specs=[vmem_spec] * 3,
        out_specs=hbm_spec,
        scratch_shapes=[pltpu.VMEM(w.shape, jnp.float32), pltpu.SemaphoreType.DMA],
        compiler_params=pltpu.CompilerParams(vmem_limit_bytes=VMEM_LIMIT),
        name="finish",
    )(parts, u, w)


def local(weights, moment, second, tile_rows, row_index, bucket_count):
    owners = lax.axis_size(AXES)
    tile_rows = pltpu.with_memory_space_constraint(tile_rows, pltpu.HBM)
    w, m, v = (pltpu.with_memory_space_constraint(x, pltpu.VMEM) for x in (weights, moment, second))
    packed = pack(tile_rows, row_index, bucket_count, owners)
    got = lax.all_to_all(packed, AXES, split_axis=0, concat_axis=0, tiled=True)
    new_moment, new_second, update, parts = step(got, w, m, v, owners)
    sums = lax.all_to_all(parts, AXES, split_axis=0, concat_axis=0, tiled=True)
    return (finish(sums, update, w), new_moment, new_second)


def solution(mesh):
    torus = Mesh(mesh.devices.reshape(4, 4, 4, 2), AXES)
    table, flat = P(AXES, None), P(AXES)
    return jax.shard_map(
        local,
        mesh=torus,
        in_specs=(table, table, table, table, flat, flat),
        out_specs=(table, table, table),
        check_vma=False,
    )
```

```python
import jax
import jax.numpy as jnp
from jax import lax
from jax.experimental import pallas as pl
from jax.experimental.pallas import tpu as pltpu
from jax.sharding import Mesh
from jax.sharding import PartitionSpec as P

AXES = ("rows_0", "rows_1", "dp_0", "dp_1")

beta_one = 0.9
beta_two = 0.999
epsilon = 1e-06
decay = 0.01
rate = 0.1

LANES = 128
VMEM_LIMIT = 20 * 1024 * 1024

any_spec = pl.BlockSpec(memory_space=pl.ANY)
vmem_spec = pl.BlockSpec(memory_space=pltpu.VMEM)
hbm_spec = pl.BlockSpec(memory_space=pltpu.HBM)


def in_hbm(x):
    return pltpu.with_memory_space_constraint(x, pltpu.HBM)


def in_vmem(x):
    return pltpu.with_memory_space_constraint(x, pltpu.VMEM)


def pack_body(rows, index_hbm, count_hbm, packed, index, count, sem, small):
    owners, capacity, width = packed.shape
    width -= LANES
    slots = owners * capacity
    short = [
        pltpu.make_async_copy(a, b, small.at[i])
        for i, (a, b) in enumerate(((index_hbm, index), (count_hbm, count)))
    ]
    for copy in short:
        copy.start()
    for b in range(owners):
        pltpu.make_async_copy(
            rows.at[pl.ds(b * capacity, capacity)], packed.at[b, :, pl.ds(0, width)], sem
        ).start()
    for copy in short:
        copy.wait()
    at = lax.broadcasted_iota(jnp.int32, (slots, slots), 0)
    spread = jnp.where(at == lax.broadcasted_iota(jnp.int32, (slots, slots), 1), index[...], 0)
    of = lax.broadcasted_iota(jnp.int32, (slots, owners), 0) // capacity
    counts = jnp.where(of == lax.broadcasted_iota(jnp.int32, (slots, owners), 1), count[...], 0)

    def along_lanes(x):
        x = x.astype(jnp.float32).astype(jnp.bfloat16)
        return jnp.dot(x, jnp.ones((x.shape[1], LANES), jnp.bfloat16), preferred_element_type=jnp.float32)

    slot = (lax.broadcasted_iota(jnp.int32, (slots, LANES), 0) % capacity).astype(jnp.float32)
    target = jnp.where(slot < along_lanes(counts), along_lanes(spread), -1.0)
    packed[:, :, pl.ds(width, LANES)] = target.astype(jnp.bfloat16).reshape(owners, capacity, LANES)
    whole = packed.at[:, :, pl.ds(0, width)]
    pltpu.make_async_copy(whole, whole, sem).wait()


def pack(rows, index, count, owners):
    slots, width = rows.shape
    return pl.pallas_call(
        pack_body,
        out_shape=pltpu.VMEM((owners, slots // owners, width + LANES), jnp.bfloat16),
        in_specs=[hbm_spec] * 3,
        out_specs=vmem_spec,
        scratch_shapes=[
            pltpu.VMEM((1, slots), jnp.int32),
            pltpu.VMEM((1, owners), jnp.int32),
            pltpu.SemaphoreType.DMA,
            pltpu.SemaphoreType.DMA((2,)),
        ],
        compiler_params=pltpu.CompilerParams(vmem_limit_bytes=VMEM_LIMIT),
        name="pack",
    )(*map(in_hbm, (rows, index.reshape(1, slots), count.reshape(1, owners))))


CHUNK = 512


def step_body(got, w, m, v_hbm, nm_hbm, nv_hbm, u, parts, v, nm, nv, sems, v_sems):
    owners, capacity, width = got.shape
    width -= LANES
    slots = owners * capacity
    rows = w.shape[0]
    fetches = []
    for j in range(width // CHUNK):
        at = pl.ds(j * CHUNK, CHUNK)
        fetches.append(pltpu.make_async_copy(v_hbm.at[:, at], v.at[:, at], v_sems.at[j]))
        fetches[-1].start()
    targets = got[:, :, pl.ds(width, LANES)].reshape(slots, LANES)
    first = (lax.broadcasted_iota(jnp.int32, (8, LANES), 1) == 0).astype(jnp.float32).astype(jnp.bfloat16)
    landing = lax.dot_general(first, targets, (((1,), (1,)), ((), ())), preferred_element_type=jnp.float32)
    row = lax.broadcasted_iota(jnp.int32, (rows, slots), 0).astype(jnp.float32)
    picker = jnp.where(landing[:1, :] == row, 1.0, 0.0).astype(jnp.bfloat16)
    update_sq = jnp.zeros((8, LANES), jnp.float32)
    weight_sq = jnp.zeros((8, LANES), jnp.float32)

    def add_squares(total, x):
        sq = (x * x).reshape(rows // 8, 8, CHUNK).sum(axis=0)
        for i in range(CHUNK // LANES):
            total = total + sq[:, i * LANES : (i + 1) * LANES]
        return total

    for j in range(width // CHUNK):
        at = pl.ds(j * CHUNK, CHUNK)
        arrived = got[:, :, at].reshape(slots, CHUNK)
        g = jnp.dot(picker, arrived, preferred_element_type=jnp.float32)
        fetches[j].wait()
        new_m = beta_one * m[:, at] + (1.0 - beta_one) * g
        new_v = beta_two * v[:, at] + (1.0 - beta_two) * g * g
        old_w = w[:, at]
        update = new_m / (jnp.sqrt(new_v) + epsilon) + decay * old_w
        nm[:, at] = new_m
        nv[:, at] = new_v
        u[:, at] = update
        for k, (a, b) in enumerate(((nm, nm_hbm), (nv, nv_hbm))):
            pltpu.make_async_copy(a.at[:, at], b.at[:, at], sems.at[k]).start()
        update_sq = add_squares(update_sq, update)
        weight_sq = add_squares(weight_sq, old_w)
    both = jnp.concatenate([x.sum(axis=0, keepdims=True) for x in (update_sq, weight_sq)], axis=1)
    parts[...] = jnp.broadcast_to(both[None], parts.shape)
    for k, (a, b) in enumerate(((nm, nm_hbm), (nv, nv_hbm))):
        pltpu.make_async_copy(a, b, sems.at[k]).wait()


def step(got, w, m, v, peers):
    table = jax.ShapeDtypeStruct(w.shape, jnp.float32)
    return pl.pallas_call(
        step_body,
        out_shape=[table, table, pltpu.VMEM(w.shape, jnp.float32), pltpu.VMEM((peers, 1, 2 * LANES), jnp.float32)],
        in_specs=[vmem_spec, vmem_spec, vmem_spec, hbm_spec],
        out_specs=[hbm_spec, hbm_spec, vmem_spec, vmem_spec],
        scratch_shapes=[pltpu.VMEM(w.shape, jnp.float32)] * 3
        + [pltpu.SemaphoreType.DMA((2,)), pltpu.SemaphoreType.DMA((w.shape[1] // CHUNK,))],
        compiler_params=pltpu.CompilerParams(vmem_limit_bytes=VMEM_LIMIT),
        name="step",
    )(got, w, m, v)


def finish_body(parts, u, w, out_hbm, out, sem):
    sums = parts[...].reshape(parts.shape[0], parts.shape[2]).sum(axis=0, keepdims=True)
    update_sq = jnp.sum(sums[:, :LANES], axis=1, keepdims=True)
    weight_sq = jnp.sum(sums[:, LANES:], axis=1, keepdims=True)
    scale = rate * (jnp.sqrt(weight_sq) / jnp.sqrt(update_sq + 1e-06))
    for i in range(out.shape[0] // 32):
        at = pl.ds(i * 32, 32)
        out[at, :] = w[at, :] - scale * u[at, :]
        pltpu.make_async_copy(out.at[at, :], out_hbm.at[at, :], sem).start()
    pltpu.make_async_copy(out, out_hbm, sem).wait()


def finish(parts, u, w):
    return pl.pallas_call(
        finish_body,
        out_shape=jax.ShapeDtypeStruct(w.shape, jnp.float32),
        in_specs=[vmem_spec] * 3,
        out_specs=hbm_spec,
        scratch_shapes=[pltpu.VMEM(w.shape, jnp.float32), pltpu.SemaphoreType.DMA],
        compiler_params=pltpu.CompilerParams(vmem_limit_bytes=VMEM_LIMIT),
        name="finish",
    )(parts, u, w)


def local(weights, moment, second, tile_rows, row_index, bucket_count):
    owners = lax.axis_size(AXES)
    w, m, v = in_vmem(weights), in_vmem(moment), in_hbm(second)
    packed = pack(tile_rows, row_index, bucket_count, owners)
    got = lax.all_to_all(packed, AXES, split_axis=0, concat_axis=0, tiled=True)
    new_moment, new_second, update, parts = step(got, w, m, v, owners)
    sums = lax.all_to_all(parts, AXES, split_axis=0, concat_axis=0, tiled=True)
    return (finish(sums, update, w), new_moment, new_second)


def solution(mesh):
    torus = Mesh(mesh.devices.reshape(4, 4, 4, 2), AXES)
    table, flat = P(AXES, None), P(AXES)
    return jax.shard_map(
        local,
        mesh=torus,
        in_specs=(table, table, table, table, flat, flat),
        out_specs=(table, table, table),
        check_vma=False,
    )
```

```python
import jax
import jax.numpy as jnp
from jax import lax
from jax.experimental import pallas as pl
from jax.experimental.pallas import tpu as pltpu
from jax.sharding import Mesh
from jax.sharding import PartitionSpec as P

AXES = ("rows_0", "rows_1", "dp_0", "dp_1")

beta_one = 0.9
beta_two = 0.999
epsilon = 1e-06
decay = 0.01
rate = 0.1

LANES = 128
VMEM_LIMIT = 20 * 1024 * 1024

any_spec = pl.BlockSpec(memory_space=pl.ANY)
vmem_spec = pl.BlockSpec(memory_space=pltpu.VMEM)
hbm_spec = pl.BlockSpec(memory_space=pltpu.HBM)


def in_hbm(x):
    return pltpu.with_memory_space_constraint(x, pltpu.HBM)


def in_vmem(x):
    return pltpu.with_memory_space_constraint(x, pltpu.VMEM)


def pack_body(rows, index_hbm, count_hbm, packed, index, count, sem, small):
    owners, capacity, width = packed.shape
    width -= LANES
    slots = owners * capacity
    short = [
        pltpu.make_async_copy(a, b, small.at[i])
        for i, (a, b) in enumerate(((index_hbm, index), (count_hbm, count)))
    ]
    for copy in short:
        copy.start()
    for b in range(owners):
        pltpu.make_async_copy(
            rows.at[pl.ds(b * capacity, capacity)], packed.at[b, :, pl.ds(0, width)], sem
        ).start()
    for copy in short:
        copy.wait()
    at = lax.broadcasted_iota(jnp.int32, (slots, slots), 0)
    spread = jnp.where(at == lax.broadcasted_iota(jnp.int32, (slots, slots), 1), index[...], 0)
    of = lax.broadcasted_iota(jnp.int32, (slots, owners), 0) // capacity
    counts = jnp.where(of == lax.broadcasted_iota(jnp.int32, (slots, owners), 1), count[...], 0)

    def along_lanes(x):
        x = x.astype(jnp.float32).astype(jnp.bfloat16)
        return jnp.dot(x, jnp.ones((x.shape[1], LANES), jnp.bfloat16), preferred_element_type=jnp.float32)

    slot = (lax.broadcasted_iota(jnp.int32, (slots, LANES), 0) % capacity).astype(jnp.float32)
    target = jnp.where(slot < along_lanes(counts), along_lanes(spread), -1.0)
    packed[:, :, pl.ds(width, LANES)] = target.astype(jnp.bfloat16).reshape(owners, capacity, LANES)
    whole = packed.at[:, :, pl.ds(0, width)]
    pltpu.make_async_copy(whole, whole, sem).wait()


def pack(rows, index, count, owners):
    slots, width = rows.shape
    return pl.pallas_call(
        pack_body,
        out_shape=pltpu.VMEM((owners, slots // owners, width + LANES), jnp.bfloat16),
        in_specs=[hbm_spec] * 3,
        out_specs=vmem_spec,
        scratch_shapes=[
            pltpu.VMEM((1, slots), jnp.int32),
            pltpu.VMEM((1, owners), jnp.int32),
            pltpu.SemaphoreType.DMA,
            pltpu.SemaphoreType.DMA((2,)),
        ],
        compiler_params=pltpu.CompilerParams(vmem_limit_bytes=VMEM_LIMIT),
        name="pack",
    )(*map(in_hbm, (rows, index.reshape(1, slots), count.reshape(1, owners))))


CHUNK = 512
AHEAD = 2


def chunks(width):
    starts = list(range(0, width - CHUNK, CHUNK))
    spans = [(at, CHUNK) for at in starts]
    return spans + [(width - CHUNK, CHUNK // 2), (width - CHUNK // 2, CHUNK // 2)]


def step_body(got, w, m, v_hbm, nm_hbm, nv_hbm, u, parts, v, nm, nv, grad, sems, v_sems):
    owners, capacity, width = got.shape
    width -= LANES
    slots = owners * capacity
    rows = w.shape[0]
    spans = chunks(width)

    def fetch(j):
        at = pl.ds(*spans[j])
        return pltpu.make_async_copy(v_hbm.at[:, at], v.at[:, at], v_sems.at[j])

    for j in range(AHEAD):
        fetch(j).start()
    targets = got[:, :, pl.ds(width, LANES)].reshape(slots, LANES)
    first = (lax.broadcasted_iota(jnp.int32, (8, LANES), 1) == 0).astype(jnp.float32).astype(jnp.bfloat16)
    landing = lax.dot_general(first, targets, (((1,), (1,)), ((), ())), preferred_element_type=jnp.float32)
    row = lax.broadcasted_iota(jnp.int32, (rows, slots), 0).astype(jnp.float32)
    picker = jnp.where(landing[:1, :] == row, 1.0, 0.0).astype(jnp.bfloat16)
    update_sq = jnp.zeros((8, LANES), jnp.float32)
    weight_sq = jnp.zeros((8, LANES), jnp.float32)
    for j, (start, size) in enumerate(spans):
        at = pl.ds(start, size)
        if j + AHEAD < len(spans):
            fetch(j + AHEAD).start()
        arrived = got[:, :, at].reshape(slots, size)
        grad[j % 2, :, pl.ds(0, size)] = jnp.dot(picker, arrived, preferred_element_type=jnp.float32)
        fetch(j).wait()
        for r in range(0, rows, 8):
            here = (pl.ds(r, 8), at)
            g = grad[j % 2, pl.ds(r, 8), pl.ds(0, size)]
            old_w = w[here]
            new_m = beta_one * m[here] + (1.0 - beta_one) * g
            new_v = beta_two * v[here] + (1.0 - beta_two) * g * g
            update = new_m / (new_v * lax.rsqrt(new_v) + epsilon) + decay * old_w
            nm[here] = new_m
            nv[here] = new_v
            u[here] = update
            for i in range(0, size, LANES):
                part = update[:, i : i + LANES]
                update_sq = update_sq + part * part
                part = old_w[:, i : i + LANES]
                weight_sq = weight_sq + part * part
        for k, (a, b) in enumerate(((nm, nm_hbm), (nv, nv_hbm))):
            pltpu.make_async_copy(a.at[:, at], b.at[:, at], sems.at[k]).start()
    both = jnp.concatenate([x.sum(axis=0, keepdims=True) for x in (update_sq, weight_sq)], axis=1)
    parts[...] = jnp.broadcast_to(both[None], parts.shape)
    for k, (a, b) in enumerate(((nm, nm_hbm), (nv, nv_hbm))):
        pltpu.make_async_copy(a, b, sems.at[k]).wait()


def step(got, w, m, v, peers):
    table = jax.ShapeDtypeStruct(w.shape, jnp.float32)
    return pl.pallas_call(
        step_body,
        out_shape=[table, table, pltpu.VMEM(w.shape, jnp.float32), pltpu.VMEM((peers, 1, 2 * LANES), jnp.float32)],
        in_specs=[vmem_spec, vmem_spec, vmem_spec, hbm_spec],
        out_specs=[hbm_spec, hbm_spec, vmem_spec, vmem_spec],
        scratch_shapes=[pltpu.VMEM(w.shape, jnp.float32)] * 3
        + [
            pltpu.VMEM((2, w.shape[0], CHUNK), jnp.float32),
            pltpu.SemaphoreType.DMA((2,)),
            pltpu.SemaphoreType.DMA((len(chunks(w.shape[1])),)),
        ],
        compiler_params=pltpu.CompilerParams(vmem_limit_bytes=VMEM_LIMIT),
        name="step",
    )(got, w, m, v)


def finish_body(parts, u, w, out_hbm, out, sem):
    sums = parts[...].reshape(parts.shape[0], parts.shape[2]).sum(axis=0, keepdims=True)
    update_sq = jnp.sum(sums[:, :LANES], axis=1, keepdims=True)
    weight_sq = jnp.sum(sums[:, LANES:], axis=1, keepdims=True)
    scale = rate * (jnp.sqrt(weight_sq) / jnp.sqrt(update_sq + 1e-06))
    for i in range(out.shape[0] // 32):
        at = pl.ds(i * 32, 32)
        out[at, :] = w[at, :] - scale * u[at, :]
        pltpu.make_async_copy(out.at[at, :], out_hbm.at[at, :], sem).start()
    pltpu.make_async_copy(out, out_hbm, sem).wait()


def finish(parts, u, w):
    return pl.pallas_call(
        finish_body,
        out_shape=jax.ShapeDtypeStruct(w.shape, jnp.float32),
        in_specs=[vmem_spec] * 3,
        out_specs=hbm_spec,
        scratch_shapes=[pltpu.VMEM(w.shape, jnp.float32), pltpu.SemaphoreType.DMA],
        compiler_params=pltpu.CompilerParams(vmem_limit_bytes=VMEM_LIMIT),
        name="finish",
    )(parts, u, w)


def local(weights, moment, second, tile_rows, row_index, bucket_count):
    owners = lax.axis_size(AXES)
    w, m, v = in_vmem(weights), in_vmem(moment), in_hbm(second)
    packed = pack(tile_rows, row_index, bucket_count, owners)
    got = lax.all_to_all(packed, AXES, split_axis=0, concat_axis=0, tiled=True)
    new_moment, new_second, update, parts = step(got, w, m, v, owners)
    sums = lax.all_to_all(parts, AXES, split_axis=0, concat_axis=0, tiled=True)
    return (finish(sums, update, w), new_moment, new_second)


def solution(mesh):
    torus = Mesh(mesh.devices.reshape(4, 4, 4, 2), AXES)
    table, flat = P(AXES, None), P(AXES)
    return jax.shard_map(
        local,
        mesh=torus,
        in_specs=(table, table, table, table, flat, flat),
        out_specs=(table, table, table),
        check_vma=False,
    )
```

```python
import jax
import jax.numpy as jnp
from jax import lax
from jax.experimental import pallas as pl
from jax.experimental.pallas import tpu as pltpu
from jax.sharding import Mesh
from jax.sharding import PartitionSpec as P

AXES = ("rows_0", "rows_1", "dp_0", "dp_1")

beta_one = 0.9
beta_two = 0.999
epsilon = 1e-06
decay = 0.01
rate = 0.1

LANES = 128
PACK_FLOPS = 4_000_000_000
VMEM_LIMIT = 20 * 1024 * 1024

any_spec = pl.BlockSpec(memory_space=pl.ANY)
vmem_spec = pl.BlockSpec(memory_space=pltpu.VMEM)
hbm_spec = pl.BlockSpec(memory_space=pltpu.HBM)


def in_hbm(x):
    return pltpu.with_memory_space_constraint(x, pltpu.HBM)


def in_vmem(x):
    return pltpu.with_memory_space_constraint(x, pltpu.VMEM)


def pack_body(rows, index_hbm, count_hbm, packed, index, count, sem, small):
    owners, capacity, width = packed.shape
    width -= LANES
    slots = owners * capacity
    short = [
        pltpu.make_async_copy(a, b, small.at[i])
        for i, (a, b) in enumerate(((index_hbm, index), (count_hbm, count)))
    ]
    for copy in short:
        copy.start()
    for b in range(owners):
        pltpu.make_async_copy(
            rows.at[pl.ds(b * capacity, capacity)], packed.at[b, :, pl.ds(0, width)], sem
        ).start()
    for copy in short:
        copy.wait()
    at = lax.broadcasted_iota(jnp.int32, (slots, slots), 0)
    spread = jnp.where(at == lax.broadcasted_iota(jnp.int32, (slots, slots), 1), index[...], 0)
    of = lax.broadcasted_iota(jnp.int32, (slots, owners), 0) // capacity
    counts = jnp.where(of == lax.broadcasted_iota(jnp.int32, (slots, owners), 1), count[...], 0)

    def along_lanes(x):
        x = x.astype(jnp.float32).astype(jnp.bfloat16)
        return jnp.dot(x, jnp.ones((x.shape[1], LANES), jnp.bfloat16), preferred_element_type=jnp.float32)

    slot = (lax.broadcasted_iota(jnp.int32, (slots, LANES), 0) % capacity).astype(jnp.float32)
    target = jnp.where(slot < along_lanes(counts), along_lanes(spread), -1.0)
    packed[:, :, pl.ds(width, LANES)] = target.astype(jnp.bfloat16).reshape(owners, capacity, LANES)
    whole = packed.at[:, :, pl.ds(0, width)]
    pltpu.make_async_copy(whole, whole, sem).wait()


def pack(rows, index, count, owners):
    slots, width = rows.shape
    return pl.pallas_call(
        pack_body,
        out_shape=pltpu.VMEM((owners, slots // owners, width + LANES), jnp.bfloat16),
        in_specs=[hbm_spec] * 3,
        out_specs=vmem_spec,
        scratch_shapes=[
            pltpu.VMEM((1, slots), jnp.int32),
            pltpu.VMEM((1, owners), jnp.int32),
            pltpu.SemaphoreType.DMA,
            pltpu.SemaphoreType.DMA((2,)),
        ],
        compiler_params=pltpu.CompilerParams(vmem_limit_bytes=VMEM_LIMIT),
        cost_estimate=pl.CostEstimate(flops=PACK_FLOPS, transcendentals=0, bytes_accessed=0),
        name="pack",
    )(*map(in_hbm, (rows, index.reshape(1, slots), count.reshape(1, owners))))


CHUNK = 512
LATE = 2 * CHUNK


def step_body(got, w, m, v, nm_hbm, nv_hbm, u, parts, late_m, late_v, nm, nv, grad, sems):
    owners, capacity, width = got.shape
    width -= LANES
    slots = owners * capacity
    rows = w.shape[0]
    early = width - LATE

    def gradient(j):
        arrived = got[:, :, pl.ds(j * CHUNK, CHUNK)].reshape(slots, CHUNK)
        grad[j % 2] = jnp.dot(picker, arrived, preferred_element_type=jnp.float32)

    targets = got[:, :, pl.ds(width, LANES)].reshape(slots, LANES)
    first = (lax.broadcasted_iota(jnp.int32, (8, LANES), 1) == 0).astype(jnp.float32).astype(jnp.bfloat16)
    landing = lax.dot_general(first, targets, (((1,), (1,)), ((), ())), preferred_element_type=jnp.float32)
    row = lax.broadcasted_iota(jnp.int32, (rows, slots), 0).astype(jnp.float32)
    picker = jnp.where(landing[:1, :] == row, 1.0, 0.0).astype(jnp.bfloat16)
    gradient(0)

    def add_squares(total, x):
        for i in range(0, x.shape[1], LANES):
            part = x[:, i : i + LANES]
            total = total + part * part
        return total

    weight_sq = [jnp.zeros((8, LANES), jnp.float32)] * 4
    for r in range(0, rows, 8):
        for i in range(4):
            weight_sq[i] = add_squares(weight_sq[i], w[pl.ds(r, 8), pl.ds(i * (width // 4), width // 4)])
    weight_sq = (weight_sq[0] + weight_sq[1]) + (weight_sq[2] + weight_sq[3])
    update_sq = [jnp.zeros((8, LANES), jnp.float32)] * 2
    for j in range(width // CHUNK):
        at = pl.ds(j * CHUNK, CHUNK)
        if j:
            gradient(j)
        is_early = j * CHUNK < early
        to_m, to_v = (nm, nv) if is_early else (late_m, late_v)
        to = at if is_early else pl.ds(j * CHUNK - early, CHUNK)
        for r in range(0, rows, 8):
            tile = pl.ds(r, 8)
            g = grad[j % 2, tile, :]
            new_m = beta_one * m[tile, at] + (1.0 - beta_one) * g
            new_v = beta_two * v[tile, at] + (1.0 - beta_two) * g * g
            update = new_m / (new_v * lax.rsqrt(new_v) + epsilon) + decay * w[tile, at]
            to_m[tile, to] = new_m
            to_v[tile, to] = new_v
            u[tile, at] = update
            update_sq[r // 8 % 2] = add_squares(update_sq[r // 8 % 2], update)
        if is_early:
            for k, (a, b) in enumerate(((nm, nm_hbm), (nv, nv_hbm))):
                pltpu.make_async_copy(a.at[:, at], b.at[:, at], sems.at[k]).start()
    sums = [x.sum(axis=0, keepdims=True) for x in (update_sq[0] + update_sq[1], weight_sq)]
    parts[...] = jnp.broadcast_to(jnp.concatenate(sums, axis=1)[None], parts.shape)
    for k, (a, b) in enumerate(((nm, nm_hbm), (nv, nv_hbm))):
        pltpu.make_async_copy(a, b.at[:, pl.ds(0, early)], sems.at[k]).wait()


def step(got, w, m, v, peers):
    rows, width = w.shape
    table = jax.ShapeDtypeStruct(w.shape, jnp.float32)
    late = pltpu.VMEM((rows, LATE), jnp.float32)
    return pl.pallas_call(
        step_body,
        out_shape=[table, table, pltpu.VMEM(w.shape, jnp.float32), pltpu.VMEM((peers, 1, 2 * LANES), jnp.float32), late, late],
        in_specs=[vmem_spec] * 4,
        out_specs=[hbm_spec, hbm_spec] + [vmem_spec] * 4,
        scratch_shapes=[
            pltpu.VMEM((rows, width - LATE), jnp.float32),
            pltpu.VMEM((rows, width - LATE), jnp.float32),
            pltpu.VMEM((2, rows, CHUNK), jnp.float32),
            pltpu.SemaphoreType.DMA((2,)),
        ],
        compiler_params=pltpu.CompilerParams(vmem_limit_bytes=VMEM_LIMIT),
        name="step",
    )(got, w, m, v)


def finish_body(parts, u, w, late_m, late_v, nm_in, nv_in, out_hbm, nm_hbm, nv_hbm, out, sem, late_sems):
    columns = pl.ds(nm_hbm.shape[1] - late_m.shape[1], late_m.shape[1])
    late = [
        pltpu.make_async_copy(a, b.at[:, columns], late_sems.at[i])
        for i, (a, b) in enumerate(((late_m, nm_hbm), (late_v, nv_hbm)))
    ]
    for copy in late:
        copy.start()
    sums = parts[...].reshape(parts.shape[0], parts.shape[2]).sum(axis=0, keepdims=True)
    update_sq = jnp.sum(sums[:, :LANES], axis=1, keepdims=True)
    weight_sq = jnp.sum(sums[:, LANES:], axis=1, keepdims=True)
    scale = rate * (jnp.sqrt(weight_sq) / jnp.sqrt(update_sq + 1e-06))
    block = 16
    for i in range(0, out.shape[0], block):
        for r in range(i, i + block, 8):
            tile = pl.ds(r, 8)
            out[tile, :] = w[tile, :] - scale * u[tile, :]
        at = pl.ds(i, block)
        pltpu.make_async_copy(out.at[at, :], out_hbm.at[at, :], sem).start()
    for copy in late:
        copy.wait()
    pltpu.make_async_copy(out, out_hbm, sem).wait()


def finish(parts, u, w, late_m, late_v, new_moment, new_second):
    table = jax.ShapeDtypeStruct(w.shape, jnp.float32)
    return pl.pallas_call(
        finish_body,
        out_shape=[table] * 3,
        in_specs=[vmem_spec] * 5 + [hbm_spec] * 2,
        out_specs=[hbm_spec] * 3,
        input_output_aliases={5: 1, 6: 2},
        scratch_shapes=[
            pltpu.VMEM(w.shape, jnp.float32),
            pltpu.SemaphoreType.DMA,
            pltpu.SemaphoreType.DMA((2,)),
        ],
        compiler_params=pltpu.CompilerParams(vmem_limit_bytes=VMEM_LIMIT),
        name="finish",
    )(parts, u, w, late_m, late_v, new_moment, new_second)


def local(weights, moment, second, tile_rows, row_index, bucket_count):
    owners = lax.axis_size(AXES)
    w, m, v = in_vmem(weights), in_vmem(moment), in_vmem(second)
    packed = pack(tile_rows, row_index, bucket_count, owners)
    got = lax.all_to_all(packed, AXES, split_axis=0, concat_axis=0, tiled=True)
    new_moment, new_second, update, parts, late_m, late_v = step(got, w, m, v, owners)
    sums = lax.all_to_all(parts, AXES, split_axis=0, concat_axis=0, tiled=True)
    return tuple(finish(sums, update, w, late_m, late_v, new_moment, new_second))


def solution(mesh):
    torus = Mesh(mesh.devices.reshape(4, 4, 4, 2), AXES)
    table, flat = P(AXES, None), P(AXES)
    return jax.shard_map(
        local,
        mesh=torus,
        in_specs=(table, table, table, table, flat, flat),
        out_specs=(table, table, table),
        check_vma=False,
    )
```

```python
import functools

import jax
import jax.numpy as jnp
from jax import lax
from jax.experimental import pallas as pl
from jax.experimental.pallas import tpu as pltpu
from jax.sharding import Mesh
from jax.sharding import PartitionSpec as P

AXES = ("rows_0", "rows_1", "dp_0", "dp_1")
TURN = (2, 3, 0, 1)

beta_one = 0.9
beta_two = 0.999
epsilon = 1e-06
decay = 0.01
rate = 0.1

LANES = 128
PACK_FLOPS = 4_000_000_000
VMEM_LIMIT = 20 * 1024 * 1024

any_spec = pl.BlockSpec(memory_space=pl.ANY)
vmem_spec = pl.BlockSpec(memory_space=pltpu.VMEM)
hbm_spec = pl.BlockSpec(memory_space=pltpu.HBM)


def in_hbm(x):
    return pltpu.with_memory_space_constraint(x, pltpu.HBM)


def in_vmem(x):
    return pltpu.with_memory_space_constraint(x, pltpu.VMEM)


def owner_at(place, sizes):
    parts = [None] * len(sizes)
    for axis in reversed(TURN):
        parts[axis] = place & (sizes[axis] - 1)
        place = place >> (sizes[axis].bit_length() - 1)
    owner = 0
    for part, size in zip(parts, sizes):
        owner = owner * size + part
    return owner


def pack_body(sizes, rows, index_hbm, count_hbm, packed, index, count, sem, small):
    owners, capacity, width = packed.shape
    width -= LANES
    slots = owners * capacity
    short = [
        pltpu.make_async_copy(a, b, small.at[i])
        for i, (a, b) in enumerate(((index_hbm, index), (count_hbm, count)))
    ]
    for copy in short:
        copy.start()
    for b in range(owners):
        pltpu.make_async_copy(
            rows.at[pl.ds(owner_at(b, sizes) * capacity, capacity)], packed.at[b, :, pl.ds(0, width)], sem
        ).start()
    for copy in short:
        copy.wait()
    def slot_at(shape):
        at = lax.broadcasted_iota(jnp.int32, shape, 0)
        low = capacity.bit_length() - 1
        return (owner_at(at >> low, sizes) << low) + (at & (capacity - 1))

    at = slot_at((slots, owners))
    lane = lax.broadcasted_iota(jnp.int32, (slots, owners), 1)
    spread = [
        jnp.where(at == lane + i, index[:, pl.ds(i, owners)], 0) for i in range(0, slots, owners)
    ]
    of = at >> (capacity.bit_length() - 1)
    counts = jnp.where(of == lane, count[...], 0)

    def along_lanes(x):
        x = x.astype(jnp.float32).astype(jnp.bfloat16)
        return jnp.dot(x, jnp.ones((x.shape[1], LANES), jnp.bfloat16), preferred_element_type=jnp.float32)

    slot = (lax.broadcasted_iota(jnp.int32, (slots, LANES), 0) % capacity).astype(jnp.float32)
    target = jnp.where(slot < along_lanes(counts), sum(along_lanes(x) for x in spread), -1.0)
    packed[:, :, pl.ds(width, LANES)] = target.astype(jnp.bfloat16).reshape(owners, capacity, LANES)
    whole = packed.at[:, :, pl.ds(0, width)]
    pltpu.make_async_copy(whole, whole, sem).wait()


def pack(rows, index, count, owners):
    slots, width = rows.shape
    return pl.pallas_call(
        functools.partial(pack_body, tuple(lax.axis_size(a) for a in AXES)),
        out_shape=pltpu.VMEM((owners, slots // owners, width + LANES), jnp.bfloat16),
        in_specs=[hbm_spec] * 3,
        out_specs=vmem_spec,
        scratch_shapes=[
            pltpu.VMEM((1, slots), jnp.int32),
            pltpu.VMEM((1, owners), jnp.int32),
            pltpu.SemaphoreType.DMA,
            pltpu.SemaphoreType.DMA((2,)),
        ],
        compiler_params=pltpu.CompilerParams(vmem_limit_bytes=VMEM_LIMIT),
        cost_estimate=pl.CostEstimate(flops=PACK_FLOPS, transcendentals=0, bytes_accessed=0),
        name="pack",
    )(*map(in_hbm, (rows, index.reshape(1, slots), count.reshape(1, owners))))


CHUNK = 512
LATE = 2 * CHUNK


def step_body(got, w, m, v, nm_hbm, nv_hbm, u, parts, late_m, late_v, nm, nv, grad, sems):
    owners, capacity, width = got.shape
    width -= LANES
    slots = owners * capacity
    rows = w.shape[0]
    early = width - LATE

    def gradient(j):
        arrived = got[:, :, pl.ds(j * CHUNK, CHUNK)].reshape(slots, CHUNK)
        grad[j % 2] = jnp.dot(picker, arrived, preferred_element_type=jnp.float32)

    targets = got[:, :, pl.ds(width, LANES)].reshape(slots, LANES)
    first = (lax.broadcasted_iota(jnp.int32, (8, LANES), 1) == 0).astype(jnp.float32).astype(jnp.bfloat16)
    landing = lax.dot_general(first, targets, (((1,), (1,)), ((), ())), preferred_element_type=jnp.float32)
    row = lax.broadcasted_iota(jnp.int32, (rows, slots), 0).astype(jnp.float32)
    picker = jnp.where(landing[:1, :] == row, 1.0, 0.0).astype(jnp.bfloat16)
    gradient(0)

    def add_squares(total, x):
        for i in range(0, x.shape[1], LANES):
            part = x[:, i : i + LANES]
            total = total + part * part
        return total

    weight_sq = [jnp.zeros((8, LANES), jnp.float32)] * 4
    for r in range(0, rows, 8):
        for i in range(4):
            weight_sq[i] = add_squares(weight_sq[i], w[pl.ds(r, 8), pl.ds(i * (width // 4), width // 4)])
    weight_sq = (weight_sq[0] + weight_sq[1]) + (weight_sq[2] + weight_sq[3])
    update_sq = [jnp.zeros((8, LANES), jnp.float32)] * 2
    for j in range(width // CHUNK):
        at = pl.ds(j * CHUNK, CHUNK)
        if j:
            gradient(j)
        is_early = j * CHUNK < early
        to_m, to_v = (nm, nv) if is_early else (late_m, late_v)
        to = at if is_early else pl.ds(j * CHUNK - early, CHUNK)
        for r in range(0, rows, 8):
            tile = pl.ds(r, 8)
            g = grad[j % 2, tile, :]
            new_m = beta_one * m[tile, at] + (1.0 - beta_one) * g
            new_v = beta_two * v[tile, at] + (1.0 - beta_two) * g * g
            update = new_m / (new_v * lax.rsqrt(new_v) + epsilon) + decay * w[tile, at]
            to_m[tile, to] = new_m
            to_v[tile, to] = new_v
            u[tile, at] = update
            update_sq[r // 8 % 2] = add_squares(update_sq[r // 8 % 2], update)
        if is_early:
            for k, (a, b) in enumerate(((nm, nm_hbm), (nv, nv_hbm))):
                pltpu.make_async_copy(a.at[:, at], b.at[:, at], sems.at[k]).start()
    sums = [x.sum(axis=0, keepdims=True) for x in (update_sq[0] + update_sq[1], weight_sq)]
    parts[...] = jnp.broadcast_to(jnp.concatenate(sums, axis=1)[None], parts.shape)
    for k, (a, b) in enumerate(((nm, nm_hbm), (nv, nv_hbm))):
        pltpu.make_async_copy(a, b.at[:, pl.ds(0, early)], sems.at[k]).wait()


def step(got, w, m, v, peers):
    rows, width = w.shape
    table = jax.ShapeDtypeStruct(w.shape, jnp.float32)
    late = pltpu.VMEM((rows, LATE), jnp.float32)
    return pl.pallas_call(
        step_body,
        out_shape=[table, table, pltpu.VMEM(w.shape, jnp.float32), pltpu.VMEM((peers, 1, 2 * LANES), jnp.float32), late, late],
        in_specs=[vmem_spec] * 4,
        out_specs=[hbm_spec, hbm_spec] + [vmem_spec] * 4,
        scratch_shapes=[
            pltpu.VMEM((rows, width - LATE), jnp.float32),
            pltpu.VMEM((rows, width - LATE), jnp.float32),
            pltpu.VMEM((2, rows, CHUNK), jnp.float32),
            pltpu.SemaphoreType.DMA((2,)),
        ],
        compiler_params=pltpu.CompilerParams(vmem_limit_bytes=VMEM_LIMIT),
        name="step",
    )(got, w, m, v)


def finish_body(parts, u, w, late_m, late_v, nm_in, nv_in, out_hbm, nm_hbm, nv_hbm, out, sem, late_sems):
    columns = pl.ds(nm_hbm.shape[1] - late_m.shape[1], late_m.shape[1])
    late = [
        pltpu.make_async_copy(a, b.at[:, columns], late_sems.at[i])
        for i, (a, b) in enumerate(((late_m, nm_hbm), (late_v, nv_hbm)))
    ]
    for copy in late:
        copy.start()
    sums = parts[...].reshape(parts.shape[0], parts.shape[2]).sum(axis=0, keepdims=True)
    update_sq = jnp.sum(sums[:, :LANES], axis=1, keepdims=True)
    weight_sq = jnp.sum(sums[:, LANES:], axis=1, keepdims=True)
    scale = rate * (jnp.sqrt(weight_sq) / jnp.sqrt(update_sq + 1e-06))
    block = 16
    for i in range(0, out.shape[0], block):
        for r in range(i, i + block, 8):
            tile = pl.ds(r, 8)
            out[tile, :] = w[tile, :] - scale * u[tile, :]
        at = pl.ds(i, block)
        pltpu.make_async_copy(out.at[at, :], out_hbm.at[at, :], sem).start()
    for copy in late:
        copy.wait()
    pltpu.make_async_copy(out, out_hbm, sem).wait()


def finish(parts, u, w, late_m, late_v, new_moment, new_second):
    table = jax.ShapeDtypeStruct(w.shape, jnp.float32)
    return pl.pallas_call(
        finish_body,
        out_shape=[table] * 3,
        in_specs=[vmem_spec] * 5 + [hbm_spec] * 2,
        out_specs=[hbm_spec] * 3,
        input_output_aliases={5: 1, 6: 2},
        scratch_shapes=[
            pltpu.VMEM(w.shape, jnp.float32),
            pltpu.SemaphoreType.DMA,
            pltpu.SemaphoreType.DMA((2,)),
        ],
        compiler_params=pltpu.CompilerParams(vmem_limit_bytes=VMEM_LIMIT),
        name="finish",
    )(parts, u, w, late_m, late_v, new_moment, new_second)


def local(weights, moment, second, tile_rows, row_index, bucket_count):
    owners = lax.axis_size(AXES)
    w, m, v = in_vmem(weights), in_vmem(moment), in_vmem(second)
    packed = pack(tile_rows, row_index, bucket_count, owners)
    got = lax.all_to_all(packed, tuple(AXES[i] for i in TURN), split_axis=0, concat_axis=0, tiled=True)
    new_moment, new_second, update, parts, late_m, late_v = step(got, w, m, v, owners)
    sums = lax.all_to_all(parts, AXES, split_axis=0, concat_axis=0, tiled=True)
    return tuple(finish(sums, update, w, late_m, late_v, new_moment, new_second))


def solution(mesh):
    torus = Mesh(mesh.devices.reshape(4, 4, 4, 2), AXES)
    table, flat = P(AXES, None), P(AXES)
    return jax.shard_map(
        local,
        mesh=torus,
        in_specs=(table, table, table, table, flat, flat),
        out_specs=(table, table, table),
        check_vma=False,
    )
```

```python
import functools

import jax
import jax.numpy as jnp
from jax import lax
from jax.experimental import pallas as pl
from jax.experimental.pallas import tpu as pltpu
from jax.sharding import Mesh
from jax.sharding import PartitionSpec as P

AXES = ("rows_0", "rows_1", "dp_0", "dp_1")
TURN = (2, 3, 1, 0)

beta_one = 0.9
beta_two = 0.999
epsilon = 1e-06
decay = 0.01
rate = 0.1

LANES = 128
GATE_FLOPS = 4_000_000_000
VMEM_LIMIT = 20 * 1024 * 1024

any_spec = pl.BlockSpec(memory_space=pl.ANY)
vmem_spec = pl.BlockSpec(memory_space=pltpu.VMEM)
hbm_spec = pl.BlockSpec(memory_space=pltpu.HBM)


def in_hbm(x):
    return pltpu.with_memory_space_constraint(x, pltpu.HBM)


def in_vmem(x):
    return pltpu.with_memory_space_constraint(x, pltpu.VMEM)


def owner_at(place, sizes):
    parts = [None] * len(sizes)
    for axis in reversed(TURN):
        parts[axis] = place & (sizes[axis] - 1)
        place = place >> (sizes[axis].bit_length() - 1)
    owner = 0
    for part, size in zip(parts, sizes):
        owner = owner * size + part
    return owner


def pack_body(sizes, rows, index_hbm, count_hbm, packed, index, count, sem, small):
    owners, capacity, width = packed.shape
    width -= LANES
    slots = owners * capacity
    short = [
        pltpu.make_async_copy(a, b, small.at[i])
        for i, (a, b) in enumerate(((index_hbm, index), (count_hbm, count)))
    ]
    for copy in short:
        copy.start()
    for b in range(owners):
        pltpu.make_async_copy(
            rows.at[pl.ds(owner_at(b, sizes) * capacity, capacity)], packed.at[b, :, pl.ds(0, width)], sem
        ).start()
    for copy in short:
        copy.wait()
    def slot_at(shape):
        at = lax.broadcasted_iota(jnp.int32, shape, 0)
        low = capacity.bit_length() - 1
        return (owner_at(at >> low, sizes) << low) + (at & (capacity - 1))

    at = slot_at((slots, owners))
    lane = lax.broadcasted_iota(jnp.int32, (slots, owners), 1)
    spread = [
        jnp.where(at == lane + i, index[:, pl.ds(i, owners)], 0) for i in range(0, slots, owners)
    ]
    of = at >> (capacity.bit_length() - 1)
    counts = jnp.where(of == lane, count[...], 0)

    def along_lanes(x):
        x = x.astype(jnp.float32).astype(jnp.bfloat16)
        return jnp.dot(x, jnp.ones((x.shape[1], LANES), jnp.bfloat16), preferred_element_type=jnp.float32)

    slot = (lax.broadcasted_iota(jnp.int32, (slots, LANES), 0) % capacity).astype(jnp.float32)
    target = jnp.where(slot < along_lanes(counts), sum(along_lanes(x) for x in spread), -1.0)
    packed[:, :, pl.ds(width, LANES)] = target.astype(jnp.bfloat16).reshape(owners, capacity, LANES)
    whole = packed.at[:, :, pl.ds(0, width)]
    pltpu.make_async_copy(whole, whole, sem).wait()


def gate_body(packed_in, packed):
    packed[0, :, pl.ds(0, LANES)] = packed_in[0, :, pl.ds(0, LANES)]


def pack(rows, index, count, owners):
    slots, width = rows.shape
    blocks = pltpu.VMEM((owners, slots // owners, width + LANES), jnp.bfloat16)
    packed = pl.pallas_call(
        functools.partial(pack_body, tuple(lax.axis_size(a) for a in AXES)),
        out_shape=blocks,
        in_specs=[hbm_spec] * 3,
        out_specs=vmem_spec,
        scratch_shapes=[
            pltpu.VMEM((1, slots), jnp.int32),
            pltpu.VMEM((1, owners), jnp.int32),
            pltpu.SemaphoreType.DMA,
            pltpu.SemaphoreType.DMA((2,)),
        ],
        compiler_params=pltpu.CompilerParams(vmem_limit_bytes=VMEM_LIMIT),
        name="pack",
    )(*map(in_hbm, (rows, index.reshape(1, slots), count.reshape(1, owners))))
    return pl.pallas_call(
        gate_body,
        out_shape=blocks,
        in_specs=[vmem_spec],
        out_specs=vmem_spec,
        input_output_aliases={0: 0},
        compiler_params=pltpu.CompilerParams(vmem_limit_bytes=VMEM_LIMIT),
        cost_estimate=pl.CostEstimate(flops=GATE_FLOPS, transcendentals=0, bytes_accessed=0),
        name="gate",
    )(packed)


CHUNK = 512
LATE = 2 * CHUNK


def step_body(got, w, m, v, nm_hbm, nv_hbm, u, parts, late_m, late_v, nm, nv, grad, sems):
    owners, capacity, width = got.shape
    width -= LANES
    slots = owners * capacity
    rows = w.shape[0]
    early = width - LATE

    def gradient(j):
        arrived = got[:, :, pl.ds(j * CHUNK, CHUNK)].reshape(slots, CHUNK)
        grad[j % 2] = jnp.dot(picker, arrived, preferred_element_type=jnp.float32)

    targets = got[:, :, pl.ds(width, LANES)].reshape(slots, LANES)
    first = (lax.broadcasted_iota(jnp.int32, (8, LANES), 1) == 0).astype(jnp.float32).astype(jnp.bfloat16)
    landing = lax.dot_general(first, targets, (((1,), (1,)), ((), ())), preferred_element_type=jnp.float32)
    row = lax.broadcasted_iota(jnp.int32, (rows, slots), 0).astype(jnp.float32)
    picker = jnp.where(landing[:1, :] == row, 1.0, 0.0).astype(jnp.bfloat16)
    gradient(0)

    def add_squares(total, x):
        for i in range(0, x.shape[1], LANES):
            part = x[:, i : i + LANES]
            total = total + part * part
        return total

    weight_sq = [jnp.zeros((8, LANES), jnp.float32)] * 4
    for r in range(0, rows, 8):
        for i in range(4):
            weight_sq[i] = add_squares(weight_sq[i], w[pl.ds(r, 8), pl.ds(i * (width // 4), width // 4)])
    weight_sq = (weight_sq[0] + weight_sq[1]) + (weight_sq[2] + weight_sq[3])
    update_sq = [jnp.zeros((8, LANES), jnp.float32)] * 2
    for j in range(width // CHUNK):
        at = pl.ds(j * CHUNK, CHUNK)
        if j:
            gradient(j)
        is_early = j * CHUNK < early
        to_m, to_v = (nm, nv) if is_early else (late_m, late_v)
        to = at if is_early else pl.ds(j * CHUNK - early, CHUNK)
        for r in range(0, rows, 8):
            tile = pl.ds(r, 8)
            g = grad[j % 2, tile, :]
            new_m = beta_one * m[tile, at] + (1.0 - beta_one) * g
            new_v = beta_two * v[tile, at] + (1.0 - beta_two) * g * g
            update = new_m / (new_v * lax.rsqrt(new_v) + epsilon) + decay * w[tile, at]
            to_m[tile, to] = new_m
            to_v[tile, to] = new_v
            u[tile, at] = update
            update_sq[r // 8 % 2] = add_squares(update_sq[r // 8 % 2], update)
        if is_early:
            for k, (a, b) in enumerate(((nm, nm_hbm), (nv, nv_hbm))):
                pltpu.make_async_copy(a.at[:, at], b.at[:, at], sems.at[k]).start()
    sums = [x.sum(axis=0, keepdims=True) for x in (update_sq[0] + update_sq[1], weight_sq)]
    parts[...] = jnp.broadcast_to(jnp.concatenate(sums, axis=1)[None], parts.shape)
    for k, (a, b) in enumerate(((nm, nm_hbm), (nv, nv_hbm))):
        pltpu.make_async_copy(a, b.at[:, pl.ds(0, early)], sems.at[k]).wait()


def step(got, w, m, v, peers):
    rows, width = w.shape
    table = jax.ShapeDtypeStruct(w.shape, jnp.float32)
    late = pltpu.VMEM((rows, LATE), jnp.float32)
    return pl.pallas_call(
        step_body,
        out_shape=[table, table, pltpu.VMEM(w.shape, jnp.float32), pltpu.VMEM((peers, 1, 2 * LANES), jnp.float32), late, late],
        in_specs=[vmem_spec] * 4,
        out_specs=[hbm_spec, hbm_spec] + [vmem_spec] * 4,
        scratch_shapes=[
            pltpu.VMEM((rows, width - LATE), jnp.float32),
            pltpu.VMEM((rows, width - LATE), jnp.float32),
            pltpu.VMEM((2, rows, CHUNK), jnp.float32),
            pltpu.SemaphoreType.DMA((2,)),
        ],
        compiler_params=pltpu.CompilerParams(vmem_limit_bytes=VMEM_LIMIT),
        name="step",
    )(got, w, m, v)


def finish_body(parts, u, w, late_m, late_v, nm_in, nv_in, out_hbm, nm_hbm, nv_hbm, out, sem, late_sems):
    columns = pl.ds(nm_hbm.shape[1] - late_m.shape[1], late_m.shape[1])
    late = [
        pltpu.make_async_copy(a, b.at[:, columns], late_sems.at[i])
        for i, (a, b) in enumerate(((late_m, nm_hbm), (late_v, nv_hbm)))
    ]
    for copy in late:
        copy.start()
    sums = parts[...].reshape(parts.shape[0], parts.shape[2]).sum(axis=0, keepdims=True)
    update_sq = jnp.sum(sums[:, :LANES], axis=1, keepdims=True)
    weight_sq = jnp.sum(sums[:, LANES:], axis=1, keepdims=True)
    scale = rate * (jnp.sqrt(weight_sq) / jnp.sqrt(update_sq + 1e-06))
    block = 16
    for i in range(0, out.shape[0], block):
        for r in range(i, i + block, 8):
            tile = pl.ds(r, 8)
            out[tile, :] = w[tile, :] - scale * u[tile, :]
        at = pl.ds(i, block)
        pltpu.make_async_copy(out.at[at, :], out_hbm.at[at, :], sem).start()
    for copy in late:
        copy.wait()
    pltpu.make_async_copy(out, out_hbm, sem).wait()


def finish(parts, u, w, late_m, late_v, new_moment, new_second):
    table = jax.ShapeDtypeStruct(w.shape, jnp.float32)
    return pl.pallas_call(
        finish_body,
        out_shape=[table] * 3,
        in_specs=[vmem_spec] * 5 + [hbm_spec] * 2,
        out_specs=[hbm_spec] * 3,
        input_output_aliases={5: 1, 6: 2},
        scratch_shapes=[
            pltpu.VMEM(w.shape, jnp.float32),
            pltpu.SemaphoreType.DMA,
            pltpu.SemaphoreType.DMA((2,)),
        ],
        compiler_params=pltpu.CompilerParams(vmem_limit_bytes=VMEM_LIMIT),
        name="finish",
    )(parts, u, w, late_m, late_v, new_moment, new_second)


def local(weights, moment, second, tile_rows, row_index, bucket_count):
    owners = lax.axis_size(AXES)
    w, m, v = in_vmem(weights), in_vmem(moment), in_vmem(second)
    packed = pack(tile_rows, row_index, bucket_count, owners)
    got = lax.all_to_all(packed, tuple(AXES[i] for i in TURN), split_axis=0, concat_axis=0, tiled=True)
    new_moment, new_second, update, parts, late_m, late_v = step(got, w, m, v, owners)
    sums = lax.all_to_all(parts, AXES, split_axis=0, concat_axis=0, tiled=True)
    return tuple(finish(sums, update, w, late_m, late_v, new_moment, new_second))


def solution(mesh):
    torus = Mesh(mesh.devices.reshape(4, 4, 4, 2), AXES)
    table, flat = P(AXES, None), P(AXES)
    return jax.shard_map(
        local,
        mesh=torus,
        in_specs=(table, table, table, table, flat, flat),
        out_specs=(table, table, table),
        check_vma=False,
    )
```

```python
import functools

import jax
import jax.numpy as jnp
from jax import lax
from jax.experimental import pallas as pl
from jax.experimental.pallas import tpu as pltpu
from jax.sharding import Mesh
from jax.sharding import PartitionSpec as P

AXES = ("rows_0", "rows_1", "dp_0", "dp_1")
TURN = (2, 3, 1, 0)

beta_one = 0.9
beta_two = 0.999
epsilon = 1e-06
decay = 0.01
rate = 0.1

LANES = 128
PACK_FLOPS = 4_000_000_000
VMEM_LIMIT = 20 * 1024 * 1024

any_spec = pl.BlockSpec(memory_space=pl.ANY)
vmem_spec = pl.BlockSpec(memory_space=pltpu.VMEM)
hbm_spec = pl.BlockSpec(memory_space=pltpu.HBM)


def in_hbm(x):
    return pltpu.with_memory_space_constraint(x, pltpu.HBM)


def in_vmem(x):
    return pltpu.with_memory_space_constraint(x, pltpu.VMEM)


def owner_at(place, sizes):
    parts = [None] * len(sizes)
    for axis in reversed(TURN):
        parts[axis] = place & (sizes[axis] - 1)
        place = place >> (sizes[axis].bit_length() - 1)
    owner = 0
    for part, size in zip(parts, sizes):
        owner = owner * size + part
    return owner


def pack_body(sizes, rows, index_hbm, count_hbm, packed, index, count, sem, small):
    owners, capacity, width = packed.shape
    width -= LANES
    slots = owners * capacity
    short = [
        pltpu.make_async_copy(a, b, small.at[i])
        for i, (a, b) in enumerate(((index_hbm, index), (count_hbm, count)))
    ]
    for copy in short:
        copy.start()
    for b in range(owners):
        pltpu.make_async_copy(
            rows.at[pl.ds(owner_at(b, sizes) * capacity, capacity)], packed.at[b, :, pl.ds(0, width)], sem
        ).start()
    for copy in short:
        copy.wait()
    def slot_at(shape):
        at = lax.broadcasted_iota(jnp.int32, shape, 0)
        low = capacity.bit_length() - 1
        return (owner_at(at >> low, sizes) << low) + (at & (capacity - 1))

    at = slot_at((slots, owners))
    lane = lax.broadcasted_iota(jnp.int32, (slots, owners), 1)
    spread = [
        jnp.where(at == lane + i, index[:, pl.ds(i, owners)], 0) for i in range(0, slots, owners)
    ]
    of = at >> (capacity.bit_length() - 1)
    counts = jnp.where(of == lane, count[...], 0)

    def along_lanes(x):
        x = x.astype(jnp.float32).astype(jnp.bfloat16)
        return jnp.dot(x, jnp.ones((x.shape[1], LANES), jnp.bfloat16), preferred_element_type=jnp.float32)

    slot = (lax.broadcasted_iota(jnp.int32, (slots, LANES), 0) % capacity).astype(jnp.float32)
    target = jnp.where(slot < along_lanes(counts), sum(along_lanes(x) for x in spread), -1.0)
    packed[:, :, pl.ds(width, LANES)] = target.astype(jnp.bfloat16).reshape(owners, capacity, LANES)
    whole = packed.at[:, :, pl.ds(0, width)]
    pltpu.make_async_copy(whole, whole, sem).wait()


def pack(rows, index, count, owners):
    slots, width = rows.shape
    return pl.pallas_call(
        functools.partial(pack_body, tuple(lax.axis_size(a) for a in AXES)),
        out_shape=pltpu.VMEM((owners, slots // owners, width + LANES), jnp.bfloat16),
        in_specs=[hbm_spec] * 3,
        out_specs=vmem_spec,
        scratch_shapes=[
            pltpu.VMEM((1, slots), jnp.int32),
            pltpu.VMEM((1, owners), jnp.int32),
            pltpu.SemaphoreType.DMA,
            pltpu.SemaphoreType.DMA((2,)),
        ],
        compiler_params=pltpu.CompilerParams(vmem_limit_bytes=VMEM_LIMIT),
        cost_estimate=pl.CostEstimate(flops=PACK_FLOPS, transcendentals=0, bytes_accessed=0),
        name="pack",
    )(*map(in_hbm, (rows, index.reshape(1, slots), count.reshape(1, owners))))


CHUNK = 512
LATE = 2 * CHUNK


def step_body(got, w, m, v, nm_hbm, nv_hbm, u, parts, late_m, late_v, nm, nv, grad, sems):
    owners, capacity, width = got.shape
    width -= LANES
    slots = owners * capacity
    rows = w.shape[0]
    early = width - LATE

    def gradient(j):
        arrived = got[:, :, pl.ds(j * CHUNK, CHUNK)].reshape(slots, CHUNK)
        grad[j % 2] = jnp.dot(picker, arrived, preferred_element_type=jnp.float32)

    targets = got[:, :, pl.ds(width, LANES)].reshape(slots, LANES)
    first = (lax.broadcasted_iota(jnp.int32, (8, LANES), 1) == 0).astype(jnp.float32).astype(jnp.bfloat16)
    landing = lax.dot_general(first, targets, (((1,), (1,)), ((), ())), preferred_element_type=jnp.float32)
    row = lax.broadcasted_iota(jnp.int32, (rows, slots), 0).astype(jnp.float32)
    picker = jnp.where(landing[:1, :] == row, 1.0, 0.0).astype(jnp.bfloat16)
    gradient(0)

    def add_squares(total, x):
        for i in range(0, x.shape[1], LANES):
            part = x[:, i : i + LANES]
            total = total + part * part
        return total

    weight_sq = [jnp.zeros((8, LANES), jnp.float32)] * 4
    for r in range(0, rows, 8):
        for i in range(4):
            weight_sq[i] = add_squares(weight_sq[i], w[pl.ds(r, 8), pl.ds(i * (width // 4), width // 4)])
    weight_sq = (weight_sq[0] + weight_sq[1]) + (weight_sq[2] + weight_sq[3])
    update_sq = [jnp.zeros((8, LANES), jnp.float32)] * 2
    for j in range(width // CHUNK):
        at = pl.ds(j * CHUNK, CHUNK)
        if j:
            gradient(j)
        is_early = j * CHUNK < early
        to_m, to_v = (nm, nv) if is_early else (late_m, late_v)
        to = at if is_early else pl.ds(j * CHUNK - early, CHUNK)
        for r in range(0, rows, 8):
            tile = pl.ds(r, 8)
            g = grad[j % 2, tile, :]
            new_m = beta_one * m[tile, at] + (1.0 - beta_one) * g
            new_v = beta_two * v[tile, at] + (1.0 - beta_two) * g * g
            update = new_m / (new_v * lax.rsqrt(new_v) + epsilon) + decay * w[tile, at]
            to_m[tile, to] = new_m
            to_v[tile, to] = new_v
            u[tile, at] = update
            update_sq[r // 8 % 2] = add_squares(update_sq[r // 8 % 2], update)
        if is_early:
            for k, (a, b) in enumerate(((nm, nm_hbm), (nv, nv_hbm))):
                pltpu.make_async_copy(a.at[:, at], b.at[:, at], sems.at[k]).start()
    sums = [x.sum(axis=0, keepdims=True) for x in (update_sq[0] + update_sq[1], weight_sq)]
    parts[...] = jnp.broadcast_to(jnp.concatenate(sums, axis=1)[None], parts.shape)
    for k, (a, b) in enumerate(((nm, nm_hbm), (nv, nv_hbm))):
        pltpu.make_async_copy(a, b.at[:, pl.ds(0, early)], sems.at[k]).wait()


def step(got, w, m, v, peers):
    rows, width = w.shape
    table = jax.ShapeDtypeStruct(w.shape, jnp.float32)
    late = pltpu.VMEM((rows, LATE), jnp.float32)
    return pl.pallas_call(
        step_body,
        out_shape=[table, table, pltpu.VMEM(w.shape, jnp.float32), pltpu.VMEM((peers, 1, 2 * LANES), jnp.float32), late, late],
        in_specs=[vmem_spec] * 4,
        out_specs=[hbm_spec, hbm_spec] + [vmem_spec] * 4,
        scratch_shapes=[
            pltpu.VMEM((rows, width - LATE), jnp.float32),
            pltpu.VMEM((rows, width - LATE), jnp.float32),
            pltpu.VMEM((2, rows, CHUNK), jnp.float32),
            pltpu.SemaphoreType.DMA((2,)),
        ],
        compiler_params=pltpu.CompilerParams(vmem_limit_bytes=VMEM_LIMIT),
        name="step",
    )(got, w, m, v)


def finish_body(parts, u, w, late_m, late_v, nm_in, nv_in, out_hbm, nm_hbm, nv_hbm, out, sem, late_sems):
    columns = pl.ds(nm_hbm.shape[1] - late_m.shape[1], late_m.shape[1])
    late = [
        pltpu.make_async_copy(a, b.at[:, columns], late_sems.at[i])
        for i, (a, b) in enumerate(((late_m, nm_hbm), (late_v, nv_hbm)))
    ]
    for copy in late:
        copy.start()
    sums = parts[...].reshape(parts.shape[0], parts.shape[2]).sum(axis=0, keepdims=True)
    update_sq = jnp.sum(sums[:, :LANES], axis=1, keepdims=True)
    weight_sq = jnp.sum(sums[:, LANES:], axis=1, keepdims=True)
    scale = rate * (jnp.sqrt(weight_sq) / jnp.sqrt(update_sq + 1e-06))
    block = 16
    for i in range(0, out.shape[0], block):
        for r in range(i, i + block, 8):
            tile = pl.ds(r, 8)
            out[tile, :] = w[tile, :] - scale * u[tile, :]
        at = pl.ds(i, block)
        pltpu.make_async_copy(out.at[at, :], out_hbm.at[at, :], sem).start()
    for copy in late:
        copy.wait()
    pltpu.make_async_copy(out, out_hbm, sem).wait()


def finish(parts, u, w, late_m, late_v, new_moment, new_second):
    table = jax.ShapeDtypeStruct(w.shape, jnp.float32)
    return pl.pallas_call(
        finish_body,
        out_shape=[table] * 3,
        in_specs=[vmem_spec] * 5 + [hbm_spec] * 2,
        out_specs=[hbm_spec] * 3,
        input_output_aliases={5: 1, 6: 2},
        scratch_shapes=[
            pltpu.VMEM(w.shape, jnp.float32),
            pltpu.SemaphoreType.DMA,
            pltpu.SemaphoreType.DMA((2,)),
        ],
        compiler_params=pltpu.CompilerParams(vmem_limit_bytes=VMEM_LIMIT),
        name="finish",
    )(parts, u, w, late_m, late_v, new_moment, new_second)


def local(weights, moment, second, tile_rows, row_index, bucket_count):
    owners = lax.axis_size(AXES)
    w, m, v = in_vmem(weights), in_vmem(moment), in_vmem(second)
    packed = pack(tile_rows, row_index, bucket_count, owners)
    got = lax.all_to_all(packed, tuple(AXES[i] for i in TURN), split_axis=0, concat_axis=0, tiled=True)
    new_moment, new_second, update, parts, late_m, late_v = step(got, w, m, v, owners)
    sums = lax.all_to_all(parts, AXES, split_axis=0, concat_axis=0, tiled=True)
    return tuple(finish(sums, update, w, late_m, late_v, new_moment, new_second))


def solution(mesh):
    torus = Mesh(mesh.devices.reshape(4, 4, 4, 2), AXES)
    table, flat = P(AXES, None), P(AXES)
    return jax.shard_map(
        local,
        mesh=torus,
        in_specs=(table, table, table, table, flat, flat),
        out_specs=(table, table, table),
        check_vma=False,
    )
```
